32 devices in a mesh: tm: 8 (over z, y), group: 4 (over x, core).
Axes of the slice: x: 2, y: 2, z: 4, core: 2. Of those that a mesh axis runs over, the one named last changes fastest.
Arguments:
- values: float32 [65536, 64], P(('tm', 'group')), may hold values from -6 to 6
- group_ids: int32 [65536], P(('tm', 'group')), may hold values from 0 to 2047, as said below
- slot_of: int32 [2048], replicated, may hold values from 0 to 2047, each once
Outputs:
- running_mean: float32 [65536, 64], P(('tm', 'group'))
- running_count: int32 [65536], P(('tm', 'group'))
- closing_mean: float32 [2048, 64], P('group')
The draws below stay inside these ranges and needn't reach their ends.
Inputs may be any that keep to these rules, and one draw needn't show every extreme that they name: `slot_of`: a permutation of the slots; slot s belongs to index s // (2048 / 4) of the group axis. `group_ids`: some store groups may have no rows in the window.
All inputs are finite; a program needn't handle non-finite values.
Results may differ from the reference program's by a relative error of at most 0.0003.
Values sent between devices are 32-bit elements; how exact they have to be, the bound alone decides.
A program may use at most 64 MiB of HBM per device.

```python
import math
import jax
import jax.numpy as jnp
from jax import lax

M = 64
G = 2048
ROWS = 65536


def draw_group_ids(key, part):
    used = G - G // 16
    order_key = jax.random.fold_in(key, 11)
    reach_key = jax.random.fold_in(key, 23)
    rank_key = jax.random.fold_in(key, 37)
    order = jax.random.permutation(order_key, G)
    reach = jax.random.randint(reach_key, (ROWS,), 1, used + 1)
    rank = jax.random.randint(rank_key, (ROWS,), 0, reach)
    return jnp.take(order, rank).astype(jnp.int32)


def block_scale(key, extent, cuts, low, largest):
    def one(dim, parts):
        draws = jax.random.uniform(jax.random.fold_in(jax.random.fold_in(key, 6), dim), (parts,), jnp.float32, low / len(cuts), largest / len(cuts))
        return jnp.repeat(jnp.exp(draws), extent[dim] // parts).reshape((-1,) + (1,) * (len(extent) - dim - 1))

    loudness = one(*cuts[0])
    for cut in cuts[1:]:
        loudness = loudness * one(*cut)
    return loudness


def bell_draw(own_key, shape, scale, most, cuts=(), kind=jnp.bfloat16):
    level = block_scale(own_key, shape, cuts, -0.22, 0.18) if cuts else 1.0
    values = jax.random.normal(own_key, shape, jnp.float32) * scale * level
    return jnp.minimum(jnp.maximum(values, -most), most).astype(kind)


def setup_inputs(seed: int = 0) -> dict:
    seeds = jax.random.split(jax.random.key(seed), 4)
    return {
        "values": bell_draw(seeds[0], (ROWS, M), 1.0, 6.0, ((0, 32),), jnp.float32),
        "group_ids": draw_group_ids(jax.random.fold_in(seeds[3], 71), 0),
        "slot_of": jax.random.permutation(seeds[2], G).astype(jnp.int32),
    }


def block_pass(values, slots, groups):
    total_rows, width = values.shape
    size = math.gcd(total_rows, 256)
    blocks = total_rows // size
    lower = jnp.arange(size)[:, None] >= jnp.arange(size)[None, :]

    def advance(carry, item):
        sums, counts = carry
        rows, keys = item
        mask = ((keys[:, None] == keys[None, :]) & lower).astype(jnp.float32)
        within = jnp.dot(mask, rows, precision=lax.Precision.HIGHEST, preferred_element_type=jnp.float32)
        inclusive = within + jnp.take(sums, keys, axis=0)
        tally = jnp.sum(mask, axis=1) + jnp.take(counts, keys)
        sums = sums + jax.ops.segment_sum(rows, keys, num_segments=groups)
        counts = counts + jax.ops.segment_sum(jnp.ones((size,), jnp.float32), keys, num_segments=groups)
        return (sums, counts), (inclusive, tally)

    start = (jnp.zeros((groups, width), jnp.float32), jnp.zeros((groups,), jnp.float32))
    final, outs = lax.scan(advance, start, (values.reshape(blocks, size, width), slots.reshape(blocks, size)))
    return final, outs[0].reshape(total_rows, width), outs[1].reshape(total_rows)


def reference(values, group_ids, slot_of):
    slots = jnp.take(slot_of, group_ids).astype(jnp.int32)
    final, running_sum, count = block_pass(values, slots, G)
    running_mean = running_sum / count[:, None]
    closing_mean = final[0] / jnp.maximum(final[1], 1.0)[:, None]
    return running_mean, count.astype(jnp.int32), closing_mean
```

```python
import functools

import jax
import jax.numpy as jnp
from jax import lax
from jax.experimental import pallas as pl
from jax.experimental.pallas import tpu as pltpu
from jax.sharding import PartitionSpec as P

MESH = pl.DeviceIdType.MESH
LANES = 128
ROWS8 = 8
F32 = jnp.float32
BF16 = jnp.bfloat16


def split_parts(x, parts):
    pieces = []
    for _ in range(parts):
        piece = x.astype(BF16).astype(F32)
        pieces.append(piece)
        x = x - piece
    return pieces


def kernel(
    na, nb, ng, count_parts, extra,
    vt_ref, ids_ref, table_ref,
    mean_ref, count_ref, closing_ref,
    lhsv, onehot, acc, lhss, mine, arrived, zbuf, back, start, shut,
    send1, recv1, sendz, recvz, send2, recv2, sendc, recvc,
):
    width, rows = vt_ref.shape
    groups = onehot.shape[0]
    plane = nb * ng
    per = groups // plane
    tm = lax.axis_index("tm")
    g_me = lax.axis_index("group")
    a_me, b_me = tm // nb, tm % nb
    p_me = b_me * ng + g_me
    o_me = g_me * nb + b_me

    def at_position(p):
        return (a_me * nb + p // ng, p % ng)

    def at_owner(o):
        return (a_me * nb + o % nb, o // nb)

    barrier = pltpu.get_barrier_semaphore()
    for k in range(1, plane):
        pl.semaphore_signal(
            barrier, inc=1, device_id=at_position((p_me + k) % plane), device_id_type=MESH
        )
    for k in range(1, na):
        pl.semaphore_signal(
            barrier, inc=1, device_id=(((a_me + k) % na) * nb + b_me, g_me), device_id_type=MESH
        )

    ids = ids_ref[...]
    low, high = ids & (LANES - 1), ids // LANES
    slots = []
    for i in range(0, ids.shape[0], ROWS8):
        index, page = low[i : i + ROWS8], high[i : i + ROWS8]
        found = jnp.zeros_like(index)
        for t in range(table_ref.shape[0]):
            entries = jnp.broadcast_to(table_ref[t : t + 1, :], index.shape)
            got = jnp.take_along_axis(entries, index, axis=1)
            found = jnp.where(page == t, got, found)
        slots.append(found)
    slots = jnp.concatenate(slots, axis=0)

    hi, lo = split_parts(vt_ref[...], 2)
    lhsv[0:width, :] = hi.astype(BF16)
    lhsv[width : 2 * width, :] = lo.astype(BF16)
    tail = jnp.where(lax.broadcasted_iota(jnp.int32, (extra, rows), 0) < ROWS8, 1.0, 0.0)
    lhsv[2 * width :, :] = tail.astype(BF16)

    pl.semaphore_wait(barrier, plane - 1 + na - 1)

    def one_chunk(o):
        base = pl.multiple_of(o * per, per)
        labels = lax.broadcasted_iota(jnp.int32, (per, LANES), 0) + o * per
        for b in range(rows // LANES):
            hit = labels == slots[b : b + 1, :]
            onehot[pl.ds(base, per), b * LANES : (b + 1) * LANES] = jnp.where(
                hit, 1.0, 0.0
            ).astype(BF16)
        sums = lax.dot_general(
            lhsv[...],
            onehot[pl.ds(base, per), :],
            (((1,), (1,)), ((), ())),
            preferred_element_type=F32,
        )
        return jnp.concatenate(
            [
                sums[0:width] + sums[width : 2 * width],
                sums[2 * width : 2 * width + ROWS8],
            ],
            axis=0,
        )

    def copy1(k, o, p):
        return pltpu.make_async_remote_copy(
            src_ref=mine.at[k],
            dst_ref=arrived.at[p],
            send_sem=send1.at[k],
            recv_sem=recv1.at[p],
            device_id=at_owner(o),
            device_id_type=MESH,
        )

    for k in range(1, plane):
        o = (o_me + k) % plane
        mine[k] = one_chunk(o)
        copy1(k, o, p_me).start()
    arrived[p_me] = one_chunk(o_me)

    step = min(rows, 2 * LANES)
    idsf = ids.astype(F32)
    columns = jnp.transpose(idsf)
    for i in range(0, rows, step):
        column = jnp.concatenate(
            [columns[:, (i + j) // LANES : (i + j) // LANES + 1] for j in range(0, step, LANES)],
            axis=0,
        )
        blocks = []
        for j in range(i, rows, LANES):
            hit = column == idsf[j // LANES : j // LANES + 1, :]
            if j < i + step:
                q = lax.broadcasted_iota(jnp.int32, (step, LANES), 0)
                r = lax.broadcasted_iota(jnp.int32, (step, LANES), 1) + (j - i)
                hit = hit & (q <= r)
            blocks.append(jnp.where(hit, 1.0, 0.0).astype(BF16))
        part = jnp.dot(
            lhsv[:, i : i + step], jnp.concatenate(blocks, axis=1), preferred_element_type=F32
        )
        if i == 0:
            acc[...] = part
        else:
            acc[:, i:] += part

    for k in range(1, plane):
        p = (p_me + plane - k) % plane
        copy1(k, o_me, p).wait_recv()
    plane_sum = arrived[0]
    for p in range(1, plane):
        plane_sum = plane_sum + arrived[p]
    zbuf[a_me] = plane_sum

    def copyz(k, a):
        return pltpu.make_async_remote_copy(
            src_ref=zbuf.at[a_me],
            dst_ref=zbuf.at[a],
            send_sem=sendz.at[k],
            recv_sem=recvz.at[a],
            device_id=(((a_me + k) % na) * nb + b_me, g_me),
            device_id_type=MESH,
        )

    for k in range(1, na):
        copyz(k, a_me).start()
    for k in range(1, na):
        copyz(k, (a_me + na - k) % na).wait_recv()
    before = jnp.zeros_like(plane_sum)
    total = jnp.zeros_like(plane_sum)
    for a in range(na):
        one = zbuf[a]
        total = total + one
        before = before + jnp.where(a < a_me, one, 0.0)

    for p in range(plane):
        back[p] = before
        if p < plane - 1:
            before = before + arrived[p]

    def copy2(k, o):
        p = (p_me + k) % plane
        return pltpu.make_async_remote_copy(
            src_ref=back.at[p],
            dst_ref=start.at[o],
            send_sem=send2.at[k],
            recv_sem=recv2.at[o],
            device_id=at_position(p),
            device_id_type=MESH,
        )

    for k in range(1, plane):
        copy2(k, o_me).start()

    shut[b_me] = total[0:width] * (1.0 / jnp.maximum(total[width : width + 1], 1.0))

    def copyc(k, b):
        return pltpu.make_async_remote_copy(
            src_ref=shut.at[b_me],
            dst_ref=shut.at[b],
            send_sem=sendc.at[k],
            recv_sem=recvc.at[b],
            device_id=(a_me * nb + (b_me + k) % nb, g_me),
            device_id_type=MESH,
        )

    for k in range(1, nb):
        copyc(k, b_me).start()

    start[o_me] = back[p_me]
    for k in range(1, plane):
        copy2(k, (o_me + plane - k) % plane).wait_recv()
    for o in range(plane):
        one = start[o]
        counts = split_parts(one[width:], count_parts)
        pad = extra // ROWS8 - count_parts
        counts = counts + [jnp.zeros_like(counts[0])] * pad
        stacked = jnp.concatenate(split_parts(one[0:width], 2) + counts, axis=0)
        lhss[:, o * per : (o + 1) * per] = stacked.astype(BF16)

    wide = min(rows, 4 * LANES)
    for i in range(0, rows, wide):
        whole = acc[:, i : i + wide] + jnp.dot(
            lhss[...], onehot[:, i : i + wide], preferred_element_type=F32
        )
        count = whole[2 * width : 2 * width + 1]
        for j in range(1, count_parts):
            count = count + whole[2 * width + j * ROWS8 : 2 * width + j * ROWS8 + 1]
        mean_ref[:, i : i + wide] = (whole[0:width] + whole[width : 2 * width]) * (1.0 / count)
        count = count.astype(jnp.int32)
        for j in range(0, wide, LANES):
            b = (i + j) // LANES
            count_ref[b : b + 1, :] = count[:, j : j + LANES]

    for k in range(1, nb):
        copyc(k, (b_me + nb - k) % nb).wait_recv()
    for b in range(nb):
        closing_ref[:, b * per : (b + 1) * per] = shut[b]

    for k in range(1, plane):
        copy1(k, (o_me + k) % plane, p_me).wait_send()
        copy2(k, o_me).wait_send()
    for k in range(1, na):
        copyz(k, a_me).wait_send()
    for k in range(1, nb):
        copyc(k, b_me).wait_send()


def inner_parts(parts, owner_slots):
    best = 1
    for n in range(1, parts + 1):
        if n * n <= parts and parts % n == 0 and owner_slots % (n * LANES) == 0:
            best = n
    return best


def solution(mesh):
    tm, ng = mesh.shape["tm"], mesh.shape["group"]

    def local(values, group_ids, slot_of):
        rows, width = values.shape
        groups = slot_of.shape[0]
        nb = inner_parts(tm, groups // ng)
        na = tm // nb
        plane = nb * ng
        per = groups // plane
        count_parts = 2 if rows * tm * ng <= 2**17 else 3
        extra = 2 * ROWS8 if count_parts == 2 else 4 * ROWS8
        tall = 2 * width + extra
        sent = width + ROWS8
        vmem = pl.BlockSpec(memory_space=pltpu.VMEM)
        dma = pltpu.SemaphoreType.DMA
        mean, count, closing = pl.pallas_call(
            functools.partial(kernel, na, nb, ng, count_parts, extra),
            out_shape=(
                jax.ShapeDtypeStruct((width, rows), F32),
                jax.ShapeDtypeStruct((rows // LANES, LANES), jnp.int32),
                jax.ShapeDtypeStruct((width, groups // ng), F32),
            ),
            in_specs=[vmem] * 3,
            out_specs=(vmem,) * 3,
            scratch_shapes=[
                pltpu.VMEM((tall, rows), BF16),
                pltpu.VMEM((groups, rows), BF16),
                pltpu.VMEM((tall, rows), F32),
                pltpu.VMEM((tall, groups), BF16),
                pltpu.VMEM((plane, sent, per), F32),
                pltpu.VMEM((plane, sent, per), F32),
                pltpu.VMEM((na, sent, per), F32),
                pltpu.VMEM((plane, sent, per), F32),
                pltpu.VMEM((plane, sent, per), F32),
                pltpu.VMEM((nb, width, per), F32),
                dma((plane,)), dma((plane,)), dma((na,)), dma((na,)),
                dma((plane,)), dma((plane,)), dma((nb,)), dma((nb,)),
            ],
            compiler_params=pltpu.CompilerParams(
                collective_id=0, has_side_effects=True, vmem_limit_bytes=60 * 1024 * 1024
            ),
            name="running_totals",
        )(
            values.T,
            group_ids.reshape(rows // LANES, LANES),
            slot_of.reshape(groups // LANES, LANES),
        )
        return mean.T, count.reshape(rows), closing.T

    in_specs = (P(("tm", "group"), None), P(("tm", "group")), P())
    out_specs = (P(("tm", "group"), None), P(("tm", "group")), P("group", None))
    return jax.shard_map(local, mesh=mesh, in_specs=in_specs, out_specs=out_specs, check_vma=False)
```

```python
import functools

import jax
import jax.numpy as jnp
from jax import lax
from jax.experimental import pallas as pl
from jax.experimental.pallas import tpu as pltpu
from jax.sharding import PartitionSpec as P

MESH = pl.DeviceIdType.MESH
LANES = 128
ROWS8 = 8
HALVES = 2
F32 = jnp.float32
BF16 = jnp.bfloat16


def split_parts(x, parts):
    pieces = []
    for _ in range(parts):
        piece = x.astype(BF16).astype(F32)
        pieces.append(piece)
        x = x - piece
    return pieces


def kernel(
    na, nb, ng, count_parts, extra,
    vt_ref, ids_ref, table_ref,
    mean_ref, count_ref, closing_ref,
    lhsv, onehot, cols, acc, lhss, mine, arrived, zbuf, back, start, shut,
    send1, recv1, sendz, recvz, send2, recv2, sendc, recvc,
):
    width, rows = vt_ref.shape
    groups = onehot.shape[0]
    plane = nb * ng
    per = groups // plane
    half = per // HALVES
    tm = lax.axis_index("tm")
    g_me = lax.axis_index("group")
    a_me, b_me = tm // nb, tm % nb
    p_me = b_me * ng + g_me
    o_me = g_me * nb + b_me

    def at_position(p):
        return (a_me * nb + p // ng, p % ng)

    def at_owner(o):
        return (a_me * nb + o % nb, o // nb)

    barrier = pltpu.get_barrier_semaphore()
    for k in range(1, plane):
        pl.semaphore_signal(
            barrier, inc=1, device_id=at_position((p_me + k) % plane), device_id_type=MESH
        )
    for k in range(1, na):
        pl.semaphore_signal(
            barrier, inc=1, device_id=(((a_me + k) % na) * nb + b_me, g_me), device_id_type=MESH
        )

    ids = ids_ref[...]
    low, high = ids & (LANES - 1), ids // LANES
    slots = []
    for i in range(0, ids.shape[0], ROWS8):
        index, page = low[i : i + ROWS8], high[i : i + ROWS8]
        found = jnp.zeros_like(index)
        for t in range(table_ref.shape[0]):
            entries = jnp.broadcast_to(table_ref[t : t + 1, :], index.shape)
            got = jnp.take_along_axis(entries, index, axis=1)
            found = jnp.where(page == t, got, found)
        slots.append(found)
    slots = jnp.concatenate(slots, axis=0)

    hi, lo = split_parts(vt_ref[...], 2)
    lhsv[0:width, :] = hi.astype(BF16)
    lhsv[width : 2 * width, :] = lo.astype(BF16)
    tail = jnp.where(lax.broadcasted_iota(jnp.int32, (extra, rows), 0) < ROWS8, 1.0, 0.0)
    lhsv[2 * width :, :] = tail.astype(BF16)

    turned = jnp.transpose(slots.astype(F32)).astype(jnp.int32)
    for b in range(rows // LANES):
        cols[b * LANES : (b + 1) * LANES, :] = jnp.broadcast_to(
            turned[:, b : b + 1], (LANES, LANES)
        )

    pl.semaphore_wait(barrier, plane - 1 + na - 1)

    def copy1(h, k, o, p):
        return pltpu.make_async_remote_copy(
            src_ref=mine.at[h, k],
            dst_ref=arrived.at[h, p],
            send_sem=send1.at[h, k],
            recv_sem=recv1.at[h, p],
            device_id=at_owner(o),
            device_id_type=MESH,
        )

    def copyz(h, k, a):
        return pltpu.make_async_remote_copy(
            src_ref=zbuf.at[h, a_me],
            dst_ref=zbuf.at[h, a],
            send_sem=sendz.at[h, k],
            recv_sem=recvz.at[h, a],
            device_id=(((a_me + k) % na) * nb + b_me, g_me),
            device_id_type=MESH,
        )

    def copy2(h, k, o):
        p = (p_me + k) % plane
        return pltpu.make_async_remote_copy(
            src_ref=back.at[h, p],
            dst_ref=start.at[h, o],
            send_sem=send2.at[h, k],
            recv_sem=recv2.at[h, o],
            device_id=at_position(p),
            device_id_type=MESH,
        )

    def copyc(h, k, b):
        return pltpu.make_async_remote_copy(
            src_ref=shut.at[h, b_me],
            dst_ref=shut.at[h, b],
            send_sem=sendc.at[h, k],
            recv_sem=recvc.at[h, b],
            device_id=(a_me * nb + (b_me + k) % nb, g_me),
            device_id_type=MESH,
        )

    order = [k % plane for k in range(1, plane + 1)]
    for h in range(HALVES):
        for first in range(0, plane, 2):
            pair = order[first : first + 2]
            masks = []
            for k in pair:
                label = lax.broadcasted_iota(jnp.int32, (1, half), 1)
                label = label + (((o_me + k) % plane) * per + h * half)
                masks.append(jnp.where(cols[:, 0:half] == label, 1.0, 0.0).astype(BF16))
            sums = jnp.dot(
                lhsv[...], jnp.concatenate(masks, axis=1), preferred_element_type=F32
            )
            for i, k in enumerate(pair):
                part = sums[:, i * half : (i + 1) * half]
                part = jnp.concatenate(
                    [
                        part[0:width] + part[width : 2 * width],
                        part[2 * width : 2 * width + ROWS8],
                    ],
                    axis=0,
                )
                if k:
                    mine[h, k] = part
                    copy1(h, k, (o_me + k) % plane, p_me).start()
                else:
                    arrived[h, p_me] = part

    def sum_plane(h):
        for k in range(1, plane):
            copy1(h, k, o_me, (p_me + plane - k) % plane).wait_recv()
        plane_sum = arrived[h, 0]
        for p in range(1, plane):
            plane_sum = plane_sum + arrived[h, p]
        zbuf[h, a_me] = plane_sum
        for k in range(1, na):
            copyz(h, k, a_me).start()

    def fill_onehot():
        for h in range(HALVES):
            for o in range(plane):
                base = (h * plane + o) * half
                labels = lax.broadcasted_iota(jnp.int32, (half, LANES), 0) + (o * per + h * half)
                for b in range(rows // LANES):
                    onehot[base : base + half, b * LANES : (b + 1) * LANES] = jnp.where(
                        labels == slots[b : b + 1, :], 1.0, 0.0
                    ).astype(BF16)

    def own_running():
        step = min(rows, 2 * LANES)
        for i in range(0, rows, step):
            column = cols[i : i + step, :]
            blocks = []
            for j in range(i, rows, LANES):
                hit = column == slots[j // LANES : j // LANES + 1, :]
                if j < i + step:
                    q = lax.broadcasted_iota(jnp.int32, (step, LANES), 0)
                    r = lax.broadcasted_iota(jnp.int32, (step, LANES), 1) + (j - i)
                    hit = hit & (q <= r)
                blocks.append(jnp.where(hit, 1.0, 0.0).astype(BF16))
            part = jnp.dot(
                lhsv[:, i : i + step], jnp.concatenate(blocks, axis=1), preferred_element_type=F32
            )
            if i == 0:
                acc[...] = part
            else:
                acc[:, i:] += part

    def send_back(h):
        for k in range(1, na):
            copyz(h, k, (a_me + na - k) % na).wait_recv()
        before = jnp.zeros((width + ROWS8, half), F32)
        for a in range(na):
            before = before + jnp.where(a < a_me, zbuf[h, a], 0.0)
        for p in range(plane):
            back[h, p] = before
            if p < plane - 1:
                before = before + arrived[h, p]
        for k in range(1, plane):
            copy2(h, k, o_me).start()
        start[h, o_me] = back[h, p_me]

    def close(h):
        total = zbuf[h, 0]
        for a in range(1, na):
            total = total + zbuf[h, a]
        shut[h, b_me] = total[0:width] * (1.0 / jnp.maximum(total[width : width + 1], 1.0))
        for k in range(1, nb):
            copyc(h, k, b_me).start()

    def take_start(h):
        for k in range(1, plane):
            copy2(h, k, (o_me + plane - k) % plane).wait_recv()
        for o in range(plane):
            one = start[h, o]
            counts = split_parts(one[width:], count_parts)
            pad = extra // ROWS8 - count_parts
            counts = counts + [jnp.zeros_like(counts[0])] * pad
            stacked = jnp.concatenate(split_parts(one[0:width], 2) + counts, axis=0)
            base = (h * plane + o) * half
            lhss[:, base : base + half] = stacked.astype(BF16)

    sum_plane(0)
    fill_onehot()
    for h in range(1, HALVES):
        sum_plane(h)
    own_running()
    for h in range(HALVES):
        send_back(h)
    for h in range(HALVES):
        close(h)

    wide = min(rows, 4 * LANES)
    deep = plane * half
    for h in range(HALVES):
        take_start(h)
        for i in range(0, rows, wide):
            whole = acc[:, i : i + wide] + jnp.dot(
                lhss[:, h * deep : (h + 1) * deep],
                onehot[h * deep : (h + 1) * deep, i : i + wide],
                preferred_element_type=F32,
            )
            if h < HALVES - 1:
                acc[:, i : i + wide] = whole
                continue
            count = whole[2 * width : 2 * width + 1]
            for j in range(1, count_parts):
                count = count + whole[2 * width + j * ROWS8 : 2 * width + j * ROWS8 + 1]
            mean_ref[:, i : i + wide] = (whole[0:width] + whole[width : 2 * width]) * (1.0 / count)
            count = count.astype(jnp.int32)
            for j in range(0, wide, LANES):
                b = (i + j) // LANES
                count_ref[b : b + 1, :] = count[:, j : j + LANES]

    for h in range(HALVES):
        for k in range(1, nb):
            copyc(h, k, (b_me + nb - k) % nb).wait_recv()
        for b in range(nb):
            at = b * per + h * half
            closing_ref[:, at : at + half] = shut[h, b]

    for h in range(HALVES):
        for k in range(1, plane):
            copy1(h, k, (o_me + k) % plane, p_me).wait_send()
            copy2(h, k, o_me).wait_send()
        for k in range(1, na):
            copyz(h, k, a_me).wait_send()
        for k in range(1, nb):
            copyc(h, k, b_me).wait_send()


def inner_parts(parts, owner_slots):
    best = 1
    for n in range(1, parts + 1):
        if n * n <= parts and parts % n == 0 and owner_slots % (n * HALVES * LANES) == 0:
            best = n
    return best


def solution(mesh):
    tm, ng = mesh.shape["tm"], mesh.shape["group"]

    def local(values, group_ids, slot_of):
        rows, width = values.shape
        groups = slot_of.shape[0]
        nb = inner_parts(tm, groups // ng)
        na = tm // nb
        plane = nb * ng
        half = groups // plane // HALVES
        count_parts = 2 if rows * tm * ng <= 2**17 else 3
        extra = 2 * ROWS8 if count_parts == 2 else 4 * ROWS8
        tall = 2 * width + extra
        sent = width + ROWS8
        vmem = pl.BlockSpec(memory_space=pltpu.VMEM)
        dma = pltpu.SemaphoreType.DMA
        mean, count, closing = pl.pallas_call(
            functools.partial(kernel, na, nb, ng, count_parts, extra),
            out_shape=(
                jax.ShapeDtypeStruct((width, rows), F32),
                jax.ShapeDtypeStruct((rows // LANES, LANES), jnp.int32),
                jax.ShapeDtypeStruct((width, groups // ng), F32),
            ),
            in_specs=[vmem] * 3,
            out_specs=(vmem,) * 3,
            scratch_shapes=[
                pltpu.VMEM((tall, rows), BF16),
                pltpu.VMEM((groups, rows), BF16),
                pltpu.VMEM((rows, LANES), jnp.int32),
                pltpu.VMEM((tall, rows), F32),
                pltpu.VMEM((tall, groups), BF16),
                pltpu.VMEM((HALVES, plane, sent, half), F32),
                pltpu.VMEM((HALVES, plane, sent, half), F32),
                pltpu.VMEM((HALVES, na, sent, half), F32),
                pltpu.VMEM((HALVES, plane, sent, half), F32),
                pltpu.VMEM((HALVES, plane, sent, half), F32),
                pltpu.VMEM((HALVES, nb, width, half), F32),
                dma((HALVES, plane)), dma((HALVES, plane)), dma((HALVES, na)), dma((HALVES, na)),
                dma((HALVES, plane)), dma((HALVES, plane)), dma((HALVES, nb)), dma((HALVES, nb)),
            ],
            compiler_params=pltpu.CompilerParams(
                collective_id=0, has_side_effects=True, vmem_limit_bytes=60 * 1024 * 1024
            ),
            name="running_totals",
        )(
            values.T,
            group_ids.reshape(rows // LANES, LANES),
            slot_of.reshape(groups // LANES, LANES),
        )
        return mean.T, count.reshape(rows), closing.T

    in_specs = (P(("tm", "group"), None), P(("tm", "group")), P())
    out_specs = (P(("tm", "group"), None), P(("tm", "group")), P("group", None))
    return jax.shard_map(local, mesh=mesh, in_specs=in_specs, out_specs=out_specs, check_vma=False)
```

```python
import functools

import jax
import jax.numpy as jnp
from jax import lax
from jax.experimental import pallas as pl
from jax.experimental.pallas import tpu as pltpu
from jax.sharding import PartitionSpec as P

MESH = pl.DeviceIdType.MESH
LANES = 128
ROWS8 = 8
HALVES = 2
F32 = jnp.float32
BF16 = jnp.bfloat16


def split_parts(x, parts):
    pieces = []
    for _ in range(parts):
        piece = x.astype(BF16).astype(F32)
        pieces.append(piece)
        x = x - piece
    return pieces


def kernel(
    na, nb, ng, count_parts, extra,
    vt_ref, ids_ref, table_ref,
    mean_ref, count_ref, closing_ref,
    lhsv, onehot, cols, acc, lhss, give, got, own, mine, arrived, zbuf, back, start, onward, came,
    shut, sendd, recvd, sendf, recvf, send1, recv1, sendz, recvz, send2, recv2, sendc, recvc,
):
    width, rows = vt_ref.shape
    groups = onehot.shape[0]
    nx = ng // 2
    pairs = nb * nx
    per = groups // (2 * pairs)
    half = per // HALVES
    tm = lax.axis_index("tm")
    g_me = lax.axis_index("group")
    a_me, b_me = tm // nb, tm % nb
    x_me, c_me = g_me // 2, g_me % 2
    c_other = 1 - c_me
    p_me = b_me * nx + x_me
    o_me = x_me * nb + b_me

    def at_position(p):
        return (a_me * nb + p // nx, 2 * (p % nx) + c_me)

    def at_owner(o):
        return (a_me * nb + o % nb, 2 * (o // nb) + c_me)

    def first_slot(o, c, h):
        return ((2 * (o // nb) + c) * nb + o % nb) * per + h * half

    partner = (tm, 2 * x_me + c_other)
    barrier = pltpu.get_barrier_semaphore()
    pl.semaphore_signal(barrier, inc=1, device_id=partner, device_id_type=MESH)
    for k in range(1, pairs):
        pl.semaphore_signal(
            barrier, inc=1, device_id=at_position((p_me + k) % pairs), device_id_type=MESH
        )
    for k in range(1, na):
        pl.semaphore_signal(
            barrier, inc=1, device_id=(((a_me + k) % na) * nb + b_me, g_me), device_id_type=MESH
        )

    ids = ids_ref[...]
    low, high = ids & (LANES - 1), ids // LANES
    slots = []
    for i in range(0, ids.shape[0], ROWS8):
        index, page = low[i : i + ROWS8], high[i : i + ROWS8]
        found = jnp.zeros_like(index)
        for t in range(table_ref.shape[0]):
            entries = jnp.broadcast_to(table_ref[t : t + 1, :], index.shape)
            hit = jnp.take_along_axis(entries, index, axis=1)
            found = jnp.where(page == t, hit, found)
        slots.append(found)
    slots = jnp.concatenate(slots, axis=0)

    hi, lo = split_parts(vt_ref[...], 2)
    lhsv[0:width, :] = hi.astype(BF16)
    lhsv[width : 2 * width, :] = lo.astype(BF16)
    tail = jnp.where(lax.broadcasted_iota(jnp.int32, (extra, rows), 0) < ROWS8, 1.0, 0.0)
    lhsv[2 * width :, :] = tail.astype(BF16)

    turned = jnp.transpose(slots.astype(F32)).astype(jnp.int32)
    for b in range(rows // LANES):
        cols[b * LANES : (b + 1) * LANES, :] = jnp.broadcast_to(
            turned[:, b : b + 1], (LANES, LANES)
        )

    pl.semaphore_wait(barrier, pairs + na - 1)

    def copyd(h):
        return pltpu.make_async_remote_copy(
            src_ref=give.at[h],
            dst_ref=got.at[h],
            send_sem=sendd.at[h],
            recv_sem=recvd.at[h],
            device_id=partner,
            device_id_type=MESH,
        )

    def copyf(h):
        return pltpu.make_async_remote_copy(
            src_ref=onward.at[h],
            dst_ref=came.at[h],
            send_sem=sendf.at[h],
            recv_sem=recvf.at[h],
            device_id=partner,
            device_id_type=MESH,
        )

    def copy1(h, k, o, p):
        return pltpu.make_async_remote_copy(
            src_ref=mine.at[h, o],
            dst_ref=arrived.at[h, p],
            send_sem=send1.at[h, k],
            recv_sem=recv1.at[h, p],
            device_id=at_owner(o),
            device_id_type=MESH,
        )

    def copyz(h, k, a):
        return pltpu.make_async_remote_copy(
            src_ref=zbuf.at[h, a_me],
            dst_ref=zbuf.at[h, a],
            send_sem=sendz.at[h, k],
            recv_sem=recvz.at[h, a],
            device_id=(((a_me + k) % na) * nb + b_me, g_me),
            device_id_type=MESH,
        )

    def copy2(h, k, o):
        p = (p_me + k) % pairs
        return pltpu.make_async_remote_copy(
            src_ref=back.at[h, p],
            dst_ref=start.at[h, o],
            send_sem=send2.at[h, k],
            recv_sem=recv2.at[h, o],
            device_id=at_position(p),
            device_id_type=MESH,
        )

    def copyc(h, k, b):
        return pltpu.make_async_remote_copy(
            src_ref=shut.at[h, b_me],
            dst_ref=shut.at[h, b],
            send_sem=sendc.at[h, k],
            recv_sem=recvc.at[h, b],
            device_id=(a_me * nb + (b_me + k) % nb, g_me),
            device_id_type=MESH,
        )

    def slot_sums(h, c, into):
        for first in range(0, pairs, 2):
            two = range(first, min(first + 2, pairs))
            masks = []
            for o in two:
                label = lax.broadcasted_iota(jnp.int32, (1, half), 1) + first_slot(o, c, h)
                masks.append(jnp.where(cols[:, 0:half] == label, 1.0, 0.0).astype(BF16))
            sums = jnp.dot(
                lhsv[...], jnp.concatenate(masks, axis=1), preferred_element_type=F32
            )
            for i, o in enumerate(two):
                part = sums[:, i * half : (i + 1) * half]
                into[h, o] = jnp.concatenate(
                    [
                        part[0:width] + part[width : 2 * width],
                        part[2 * width : 2 * width + ROWS8],
                    ],
                    axis=0,
                )

    def send_pair_sums(h):
        copyd(h).wait_recv()
        for o in range(pairs):
            mine[h, o] = own[h, o] + got[h, o]
        for k in range(1, pairs):
            copy1(h, k, (o_me + k) % pairs, p_me).start()
        arrived[h, p_me] = mine[h, o_me]

    def sum_plane(h):
        for k in range(1, pairs):
            copy1(h, k, o_me, (p_me + pairs - k) % pairs).wait_recv()
        plane_sum = arrived[h, 0]
        for p in range(1, pairs):
            plane_sum = plane_sum + arrived[h, p]
        zbuf[h, a_me] = plane_sum
        for k in range(1, na):
            copyz(h, k, a_me).start()

    def fill_onehot():
        for h in range(HALVES):
            for i, c in enumerate((c_me, c_other)):
                for o in range(pairs):
                    base = ((h * 2 + i) * pairs + o) * half
                    labels = lax.broadcasted_iota(jnp.int32, (half, LANES), 0) + first_slot(o, c, h)
                    for b in range(rows // LANES):
                        onehot[base : base + half, b * LANES : (b + 1) * LANES] = jnp.where(
                            labels == slots[b : b + 1, :], 1.0, 0.0
                        ).astype(BF16)

    def own_running():
        step = min(rows, 2 * LANES)
        for i in range(0, rows, step):
            column = cols[i : i + step, :]
            blocks = []
            for j in range(i, rows, LANES):
                hit = column == slots[j // LANES : j // LANES + 1, :]
                if j < i + step:
                    q = lax.broadcasted_iota(jnp.int32, (step, LANES), 0)
                    r = lax.broadcasted_iota(jnp.int32, (step, LANES), 1) + (j - i)
                    hit = hit & (q <= r)
                blocks.append(jnp.where(hit, 1.0, 0.0).astype(BF16))
            part = jnp.dot(
                lhsv[:, i : i + step], jnp.concatenate(blocks, axis=1), preferred_element_type=F32
            )
            if i == 0:
                acc[...] = part
            else:
                acc[:, i:] += part

    def send_back(h):
        for k in range(1, na):
            copyz(h, k, (a_me + na - k) % na).wait_recv()
        before = jnp.zeros((width + ROWS8, half), F32)
        for a in range(na):
            before = before + jnp.where(a < a_me, zbuf[h, a], 0.0)
        for p in range(pairs):
            back[h, p] = before
            if p < pairs - 1:
                before = before + arrived[h, p]
        for k in range(1, pairs):
            copy2(h, k, o_me).start()
        start[h, o_me] = back[h, p_me]

    def close(h):
        total = zbuf[h, 0]
        for a in range(1, na):
            total = total + zbuf[h, a]
        shut[h, b_me] = total[0:width] * (1.0 / jnp.maximum(total[width : width + 1], 1.0))
        for k in range(1, nb):
            copyc(h, k, b_me).start()

    def set_start(one, at):
        counts = split_parts(one[width:], count_parts)
        pad = extra // ROWS8 - count_parts
        counts = counts + [jnp.zeros_like(counts[0])] * pad
        stacked = jnp.concatenate(split_parts(one[0:width], 2) + counts, axis=0)
        lhss[:, at * half : (at + 1) * half] = stacked.astype(BF16)

    def take_start(h):
        for k in range(1, pairs):
            copy2(h, k, (o_me + pairs - k) % pairs).wait_recv()
        for o in range(pairs):
            onward[h, o] = start[h, o] + jnp.where(c_me == 0, own[h, o], 0.0)
        copyf(h).start()
        for o in range(pairs):
            set_start(start[h, o] + jnp.where(c_me == 1, got[h, o], 0.0), h * 2 * pairs + o)

    def take_other(h):
        copyf(h).wait_recv()
        for o in range(pairs):
            set_start(came[h, o], (h * 2 + 1) * pairs + o)

    wide = min(rows, 4 * LANES)
    deep = pairs * half

    def add_start(block, last):
        for i in range(0, rows, wide):
            whole = acc[:, i : i + wide] + jnp.dot(
                lhss[:, block * deep : (block + 1) * deep],
                onehot[block * deep : (block + 1) * deep, i : i + wide],
                preferred_element_type=F32,
            )
            if not last:
                acc[:, i : i + wide] = whole
                continue
            count = whole[2 * width : 2 * width + 1]
            for j in range(1, count_parts):
                count = count + whole[2 * width + j * ROWS8 : 2 * width + j * ROWS8 + 1]
            mean_ref[:, i : i + wide] = (whole[0:width] + whole[width : 2 * width]) * (1.0 / count)
            count = count.astype(jnp.int32)
            for j in range(0, wide, LANES):
                b = (i + j) // LANES
                count_ref[b : b + 1, :] = count[:, j : j + LANES]

    slot_sums(0, c_other, give)
    copyd(0).start()
    slot_sums(0, c_me, own)
    for h in range(1, HALVES):
        slot_sums(h, c_other, give)
        copyd(h).start()
        send_pair_sums(h - 1)
        slot_sums(h, c_me, own)
    send_pair_sums(HALVES - 1)
    sum_plane(0)
    fill_onehot()
    for h in range(1, HALVES):
        sum_plane(h)
    own_running()
    for h in range(HALVES):
        send_back(h)
    for h in range(HALVES):
        close(h)
    for h in range(HALVES):
        take_start(h)
        add_start(2 * h, False)
        take_other(h)
        add_start(2 * h + 1, h == HALVES - 1)

    for h in range(HALVES):
        for k in range(1, nb):
            copyc(h, k, (b_me + nb - k) % nb).wait_recv()
        for b in range(nb):
            at = b * per + h * half
            closing_ref[:, at : at + half] = shut[h, b]

    for h in range(HALVES):
        copyd(h).wait_send()
        copyf(h).wait_send()
        for k in range(1, pairs):
            copy1(h, k, (o_me + k) % pairs, p_me).wait_send()
            copy2(h, k, o_me).wait_send()
        for k in range(1, na):
            copyz(h, k, a_me).wait_send()
        for k in range(1, nb):
            copyc(h, k, b_me).wait_send()


def inner_parts(parts, owner_slots):
    best = 1
    for n in range(1, parts + 1):
        if n * n <= parts and parts % n == 0 and owner_slots % (n * HALVES * LANES) == 0:
            best = n
    return best


def solution(mesh):
    tm, ng = mesh.shape["tm"], mesh.shape["group"]

    def local(values, group_ids, slot_of):
        rows, width = values.shape
        groups = slot_of.shape[0]
        nb = inner_parts(tm, groups // ng)
        na = tm // nb
        pairs = nb * ng // 2
        half = groups // (2 * pairs) // HALVES
        count_parts = 2 if rows * tm * ng <= 2**17 else 3
        extra = 2 * ROWS8 if count_parts == 2 else 4 * ROWS8
        tall = 2 * width + extra
        sent = width + ROWS8
        vmem = pl.BlockSpec(memory_space=pltpu.VMEM)
        dma = pltpu.SemaphoreType.DMA
        mean, count, closing = pl.pallas_call(
            functools.partial(kernel, na, nb, ng, count_parts, extra),
            out_shape=(
                jax.ShapeDtypeStruct((width, rows), F32),
                jax.ShapeDtypeStruct((rows // LANES, LANES), jnp.int32),
                jax.ShapeDtypeStruct((width, groups // ng), F32),
            ),
            in_specs=[vmem] * 3,
            out_specs=(vmem,) * 3,
            scratch_shapes=[
                pltpu.VMEM((tall, rows), BF16),
                pltpu.VMEM((groups, rows), BF16),
                pltpu.VMEM((rows, LANES), jnp.int32),
                pltpu.VMEM((tall, rows), F32),
                pltpu.VMEM((tall, groups), BF16),
                pltpu.VMEM((HALVES, pairs, sent, half), F32),
                pltpu.VMEM((HALVES, pairs, sent, half), F32),
                pltpu.VMEM((HALVES, pairs, sent, half), F32),
                pltpu.VMEM((HALVES, pairs, sent, half), F32),
                pltpu.VMEM((HALVES, pairs, sent, half), F32),
                pltpu.VMEM((HALVES, na, sent, half), F32),
                pltpu.VMEM((HALVES, pairs, sent, half), F32),
                pltpu.VMEM((HALVES, pairs, sent, half), F32),
                pltpu.VMEM((HALVES, pairs, sent, half), F32),
                pltpu.VMEM((HALVES, pairs, sent, half), F32),
                pltpu.VMEM((HALVES, nb, width, half), F32),
                dma((HALVES,)), dma((HALVES,)), dma((HALVES,)), dma((HALVES,)),
                dma((HALVES, pairs)), dma((HALVES, pairs)), dma((HALVES, na)), dma((HALVES, na)),
                dma((HALVES, pairs)), dma((HALVES, pairs)), dma((HALVES, nb)), dma((HALVES, nb)),
            ],
            compiler_params=pltpu.CompilerParams(
                collective_id=0, has_side_effects=True, vmem_limit_bytes=60 * 1024 * 1024
            ),
            name="running_totals",
        )(
            values.T,
            group_ids.reshape(rows // LANES, LANES),
            slot_of.reshape(groups // LANES, LANES),
        )
        return mean.T, count.reshape(rows), closing.T

    in_specs = (P(("tm", "group"), None), P(("tm", "group")), P())
    out_specs = (P(("tm", "group"), None), P(("tm", "group")), P("group", None))
    return jax.shard_map(local, mesh=mesh, in_specs=in_specs, out_specs=out_specs, check_vma=False)
```

```python
import functools

import jax
import jax.numpy as jnp
from jax import lax
from jax.experimental import pallas as pl
from jax.experimental.pallas import tpu as pltpu
from jax.sharding import PartitionSpec as P

MESH = pl.DeviceIdType.MESH
LANES = 128
ROWS8 = 8
HALVES = 2
F32 = jnp.float32
BF16 = jnp.bfloat16


def split_parts(x, parts):
    pieces = []
    for _ in range(parts):
        piece = x.astype(BF16).astype(F32)
        pieces.append(piece)
        x = x - piece
    return pieces


def kernel(
    na, nb, ng, count_parts, extra,
    vt_ref, ids_ref, table_ref,
    mean_ref, count_ref, closing_ref,
    lhsv, onehot, cols, acc, lhss, give, got, own, mine, arrived, zbuf, zgot, back, start, onward, came,
    shut, sendd, recvd, sendf, recvf, send1, recv1, sendz, recvz, send2, recv2, sendc, recvc,
):
    width, rows = vt_ref.shape
    groups = onehot.shape[0]
    nx = ng // 2
    pairs = nb * nx
    per = groups // (2 * pairs)
    half = per // HALVES
    tm = lax.axis_index("tm")
    g_me = lax.axis_index("group")
    a_me, b_me = tm // nb, tm % nb
    x_me, c_me = g_me // 2, g_me % 2
    c_other = 1 - c_me
    p_me = b_me * nx + x_me
    o_me = x_me * nb + b_me

    def at_position(p):
        return (a_me * nb + p // nx, 2 * (p % nx) + c_me)

    def at_owner(o):
        return (a_me * nb + o % nb, 2 * (o // nb) + c_me)

    def first_slot(o, c, h):
        return ((2 * (o // nb) + c) * nb + o % nb) * per + h * half

    partner = (tm, 2 * x_me + c_other)
    levels = na.bit_length() - 1

    def across(t):
        upper = (a_me // 2**t) % 2
        return ((a_me + 2**t * (1 - 2 * upper)) * nb + b_me, g_me)

    barrier = pltpu.get_barrier_semaphore()
    pl.semaphore_signal(barrier, inc=1, device_id=partner, device_id_type=MESH)
    for k in range(1, pairs):
        pl.semaphore_signal(
            barrier, inc=1, device_id=at_position((p_me + k) % pairs), device_id_type=MESH
        )
    for t in range(levels):
        pl.semaphore_signal(barrier, inc=1, device_id=across(t), device_id_type=MESH)

    ids = ids_ref[...]
    low, high = ids & (LANES - 1), ids // LANES
    slots = []
    for i in range(0, ids.shape[0], ROWS8):
        index, page = low[i : i + ROWS8], high[i : i + ROWS8]
        found = jnp.zeros_like(index)
        for t in range(table_ref.shape[0]):
            entries = jnp.broadcast_to(table_ref[t : t + 1, :], index.shape)
            hit = jnp.take_along_axis(entries, index, axis=1)
            found = jnp.where(page == t, hit, found)
        slots.append(found)
    slots = jnp.concatenate(slots, axis=0)

    hi, lo = split_parts(vt_ref[...], 2)
    lhsv[0:width, :] = hi.astype(BF16)
    lhsv[width : 2 * width, :] = lo.astype(BF16)
    tail = jnp.where(lax.broadcasted_iota(jnp.int32, (extra, rows), 0) < ROWS8, 1.0, 0.0)
    lhsv[2 * width :, :] = tail.astype(BF16)

    turned = jnp.transpose(slots.astype(F32)).astype(jnp.int32)
    for b in range(rows // LANES):
        cols[b * LANES : (b + 1) * LANES, :] = jnp.broadcast_to(
            turned[:, b : b + 1], (LANES, LANES)
        )

    pl.semaphore_wait(barrier, pairs + levels)

    def copyd(h):
        return pltpu.make_async_remote_copy(
            src_ref=give.at[h],
            dst_ref=got.at[h],
            send_sem=sendd.at[h],
            recv_sem=recvd.at[h],
            device_id=partner,
            device_id_type=MESH,
        )

    def copyf(h):
        return pltpu.make_async_remote_copy(
            src_ref=onward.at[h],
            dst_ref=came.at[h],
            send_sem=sendf.at[h],
            recv_sem=recvf.at[h],
            device_id=partner,
            device_id_type=MESH,
        )

    def copy1(h, k, o, p):
        return pltpu.make_async_remote_copy(
            src_ref=mine.at[h, o],
            dst_ref=arrived.at[h, p],
            send_sem=send1.at[h, k],
            recv_sem=recv1.at[h, p],
            device_id=at_owner(o),
            device_id_type=MESH,
        )

    def copyz(h, t):
        return pltpu.make_async_remote_copy(
            src_ref=zbuf.at[h, t],
            dst_ref=zgot.at[h, t],
            send_sem=sendz.at[h, t],
            recv_sem=recvz.at[h, t],
            device_id=across(t),
            device_id_type=MESH,
        )

    def copy2(h, k, o):
        p = (p_me + k) % pairs
        return pltpu.make_async_remote_copy(
            src_ref=back.at[h, p],
            dst_ref=start.at[h, o],
            send_sem=send2.at[h, k],
            recv_sem=recv2.at[h, o],
            device_id=at_position(p),
            device_id_type=MESH,
        )

    def copyc(h, k, b):
        return pltpu.make_async_remote_copy(
            src_ref=shut.at[h, b_me],
            dst_ref=shut.at[h, b],
            send_sem=sendc.at[h, k],
            recv_sem=recvc.at[h, b],
            device_id=(a_me * nb + (b_me + k) % nb, g_me),
            device_id_type=MESH,
        )

    def slot_sums(h, c, into):
        for first in range(0, pairs, 2):
            two = range(first, min(first + 2, pairs))
            masks = []
            for o in two:
                label = lax.broadcasted_iota(jnp.int32, (1, half), 1) + first_slot(o, c, h)
                masks.append(jnp.where(cols[:, 0:half] == label, 1.0, 0.0).astype(BF16))
            sums = jnp.dot(
                lhsv[...], jnp.concatenate(masks, axis=1), preferred_element_type=F32
            )
            for i, o in enumerate(two):
                part = sums[:, i * half : (i + 1) * half]
                into[h, o] = jnp.concatenate(
                    [
                        part[0:width] + part[width : 2 * width],
                        part[2 * width : 2 * width + ROWS8],
                    ],
                    axis=0,
                )

    def send_pair_sums(h):
        copyd(h).wait_recv()
        for o in range(pairs):
            mine[h, o] = own[h, o] + got[h, o]
        for k in range(1, pairs):
            copy1(h, k, (o_me + k) % pairs, p_me).start()
        arrived[h, p_me] = mine[h, o_me]

    def sum_plane(h):
        for k in range(1, pairs):
            copy1(h, k, o_me, (p_me + pairs - k) % pairs).wait_recv()
        plane_sum = arrived[h, 0]
        for p in range(1, pairs):
            plane_sum = plane_sum + arrived[h, p]
        zbuf[h, 0] = plane_sum
        if levels:
            copyz(h, 0).start()

    def double(h, t):
        copyz(h, t).wait_recv()
        zbuf[h, t + 1] = zbuf[h, t] + zgot[h, t]
        if t + 1 < levels:
            copyz(h, t + 1).start()

    def fill_onehot():
        for h in range(HALVES):
            for i, c in enumerate((c_me, c_other)):
                for o in range(pairs):
                    base = ((h * 2 + i) * pairs + o) * half
                    labels = lax.broadcasted_iota(jnp.int32, (half, LANES), 0) + first_slot(o, c, h)
                    for b in range(rows // LANES):
                        onehot[base : base + half, b * LANES : (b + 1) * LANES] = jnp.where(
                            labels == slots[b : b + 1, :], 1.0, 0.0
                        ).astype(BF16)

    def own_running():
        step = min(rows, 2 * LANES)
        for i in range(0, rows, step):
            column = cols[i : i + step, :]
            blocks = []
            for j in range(i, rows, LANES):
                hit = column == slots[j // LANES : j // LANES + 1, :]
                if j < i + step:
                    q = lax.broadcasted_iota(jnp.int32, (step, LANES), 0)
                    r = lax.broadcasted_iota(jnp.int32, (step, LANES), 1) + (j - i)
                    hit = hit & (q <= r)
                blocks.append(jnp.where(hit, 1.0, 0.0).astype(BF16))
            part = jnp.dot(
                lhsv[:, i : i + step], jnp.concatenate(blocks, axis=1), preferred_element_type=F32
            )
            if i == 0:
                acc[...] = part
            else:
                acc[:, i:] += part

    def send_back(h):
        for t in range(1, levels):
            double(h, t)
        before = jnp.zeros((width + ROWS8, half), F32)
        for t in range(levels):
            before = before + jnp.where((a_me // 2**t) % 2 == 1, zgot[h, t], 0.0)
        for p in range(pairs):
            back[h, p] = before
            if p < pairs - 1:
                before = before + arrived[h, p]
        for k in range(1, pairs):
            copy2(h, k, o_me).start()
        start[h, o_me] = back[h, p_me]

    def close(h):
        total = zbuf[h, levels]
        shut[h, b_me] = total[0:width] * (1.0 / jnp.maximum(total[width : width + 1], 1.0))
        for k in range(1, nb):
            copyc(h, k, b_me).start()

    def set_start(one, at):
        counts = split_parts(one[width:], count_parts)
        pad = extra // ROWS8 - count_parts
        counts = counts + [jnp.zeros_like(counts[0])] * pad
        stacked = jnp.concatenate(split_parts(one[0:width], 2) + counts, axis=0)
        lhss[:, at * half : (at + 1) * half] = stacked.astype(BF16)

    def take_start(h):
        for k in range(1, pairs):
            copy2(h, k, (o_me + pairs - k) % pairs).wait_recv()
        for o in range(pairs):
            onward[h, o] = start[h, o] + jnp.where(c_me == 0, own[h, o], 0.0)
        copyf(h).start()
        for o in range(pairs):
            set_start(start[h, o] + jnp.where(c_me == 1, got[h, o], 0.0), h * 2 * pairs + o)

    def take_other(h):
        copyf(h).wait_recv()
        for o in range(pairs):
            set_start(came[h, o], (h * 2 + 1) * pairs + o)

    wide = min(rows, 4 * LANES)
    deep = pairs * half

    def add_start(block, last):
        for i in range(0, rows, wide):
            whole = acc[:, i : i + wide] + jnp.dot(
                lhss[:, block * deep : (block + 1) * deep],
                onehot[block * deep : (block + 1) * deep, i : i + wide],
                preferred_element_type=F32,
            )
            if not last:
                acc[:, i : i + wide] = whole
                continue
            count = whole[2 * width : 2 * width + 1]
            for j in range(1, count_parts):
                count = count + whole[2 * width + j * ROWS8 : 2 * width + j * ROWS8 + 1]
            mean_ref[:, i : i + wide] = (whole[0:width] + whole[width : 2 * width]) * (1.0 / count)
            count = count.astype(jnp.int32)
            for j in range(0, wide, LANES):
                b = (i + j) // LANES
                count_ref[b : b + 1, :] = count[:, j : j + LANES]

    slot_sums(0, c_other, give)
    copyd(0).start()
    slot_sums(0, c_me, own)
    for h in range(1, HALVES):
        slot_sums(h, c_other, give)
        copyd(h).start()
        send_pair_sums(h - 1)
        slot_sums(h, c_me, own)
    send_pair_sums(HALVES - 1)
    sum_plane(0)
    fill_onehot()
    for h in range(1, HALVES):
        sum_plane(h)
        if levels:
            double(h - 1, 0)
    own_running()
    if levels:
        double(HALVES - 1, 0)
    for h in range(HALVES):
        send_back(h)
    for h in range(HALVES):
        close(h)
    for h in range(HALVES):
        take_start(h)
        add_start(2 * h, False)
        take_other(h)
        add_start(2 * h + 1, h == HALVES - 1)

    for h in range(HALVES):
        for k in range(1, nb):
            copyc(h, k, (b_me + nb - k) % nb).wait_recv()
        for b in range(nb):
            at = b * per + h * half
            closing_ref[:, at : at + half] = shut[h, b]

    for h in range(HALVES):
        copyd(h).wait_send()
        copyf(h).wait_send()
        for k in range(1, pairs):
            copy1(h, k, (o_me + k) % pairs, p_me).wait_send()
            copy2(h, k, o_me).wait_send()
        for t in range(levels):
            copyz(h, t).wait_send()
        for k in range(1, nb):
            copyc(h, k, b_me).wait_send()


def inner_parts(parts, owner_slots):
    best = 1
    for n in range(1, parts + 1):
        if n * n <= parts and parts % n == 0 and owner_slots % (n * HALVES * LANES) == 0:
            best = n
    return best


def solution(mesh):
    tm, ng = mesh.shape["tm"], mesh.shape["group"]

    def local(values, group_ids, slot_of):
        rows, width = values.shape
        groups = slot_of.shape[0]
        nb = inner_parts(tm, groups // ng)
        na = tm // nb
        assert na & (na - 1) == 0
        steps = na.bit_length() - 1
        pairs = nb * ng // 2
        half = groups // (2 * pairs) // HALVES
        count_parts = 2 if rows * tm * ng <= 2**17 else 3
        extra = 2 * ROWS8 if count_parts == 2 else 4 * ROWS8
        tall = 2 * width + extra
        sent = width + ROWS8
        vmem = pl.BlockSpec(memory_space=pltpu.VMEM)
        dma = pltpu.SemaphoreType.DMA
        mean, count, closing = pl.pallas_call(
            functools.partial(kernel, na, nb, ng, count_parts, extra),
            out_shape=(
                jax.ShapeDtypeStruct((width, rows), F32),
                jax.ShapeDtypeStruct((rows // LANES, LANES), jnp.int32),
                jax.ShapeDtypeStruct((width, groups // ng), F32),
            ),
            in_specs=[vmem] * 3,
            out_specs=(vmem,) * 3,
            scratch_shapes=[
                pltpu.VMEM((tall, rows), BF16),
                pltpu.VMEM((groups, rows), BF16),
                pltpu.VMEM((rows, LANES), jnp.int32),
                pltpu.VMEM((tall, rows), F32),
                pltpu.VMEM((tall, groups), BF16),
                pltpu.VMEM((HALVES, pairs, sent, half), F32),
                pltpu.VMEM((HALVES, pairs, sent, half), F32),
                pltpu.VMEM((HALVES, pairs, sent, half), F32),
                pltpu.VMEM((HALVES, pairs, sent, half), F32),
                pltpu.VMEM((HALVES, pairs, sent, half), F32),
                pltpu.VMEM((HALVES, steps + 1, sent, half), F32),
                pltpu.VMEM((HALVES, max(steps, 1), sent, half), F32),
                pltpu.VMEM((HALVES, pairs, sent, half), F32),
                pltpu.VMEM((HALVES, pairs, sent, half), F32),
                pltpu.VMEM((HALVES, pairs, sent, half), F32),
                pltpu.VMEM((HALVES, pairs, sent, half), F32),
                pltpu.VMEM((HALVES, nb, width, half), F32),
                dma((HALVES,)), dma((HALVES,)), dma((HALVES,)), dma((HALVES,)),
                dma((HALVES, pairs)), dma((HALVES, pairs)), dma((HALVES, max(steps, 1))), dma((HALVES, max(steps, 1))),
                dma((HALVES, pairs)), dma((HALVES, pairs)), dma((HALVES, nb)), dma((HALVES, nb)),
            ],
            compiler_params=pltpu.CompilerParams(
                collective_id=0, has_side_effects=True, vmem_limit_bytes=60 * 1024 * 1024
            ),
            name="running_totals",
        )(
            values.T,
            group_ids.reshape(rows // LANES, LANES),
            slot_of.reshape(groups // LANES, LANES),
        )
        return mean.T, count.reshape(rows), closing.T

    in_specs = (P(("tm", "group"), None), P(("tm", "group")), P())
    out_specs = (P(("tm", "group"), None), P(("tm", "group")), P("group", None))
    return jax.shard_map(local, mesh=mesh, in_specs=in_specs, out_specs=out_specs, check_vma=False)
```
